32 devices in a mesh: lat: 8 (over y, x, core), blk: 4 (over z).
Axes of the slice: x: 2, y: 2, z: 4, core: 2. Of those that a mesh axis runs over, the one named last changes fastest.
Arguments:
- mesh_nodes: bfloat16 [10240, 512], P(('lat', 'blk')), may hold values from -6 to 6
- coarse_nodes: bfloat16 [640, 512], replicated, may hold values from -6 to 6
- edge_latents: bfloat16 [65536, 512], P(('lat', 'blk')), may hold values from -6 to 6
- edge_tiles: int32 [512, 2, 128], P(('lat', 'blk')), may hold values from 0 to 1023, as said below
- send_lists: int32 [32, 8, 8], P(('lat', 'blk')), may hold values from 0 to 319
- tiles_live: int32 [32], P(('lat', 'blk')), may hold values from 1 to 16, as said below
- edge_in: bfloat16 [3, 512, 512], replicated, may hold values from -0.15625 to 0.15625
- edge_out: bfloat16 [512, 512], replicated, may hold values from -0.25 to 0.25
- edge_gain: float32 [512], replicated, may hold values from 0.1 to 1.9
- node_in: bfloat16 [2, 512, 512], replicated, may hold values from -0.1875 to 0.1875
- node_out: bfloat16 [512, 512], replicated, may hold values from -0.25 to 0.25
- node_gain: float32 [512], replicated, may hold values from 0.1 to 1.9
- grad_nodes: bfloat16 [10240, 512], P(('lat', 'blk')), may hold values from -6 to 6
- grad_coarse: bfloat16 [640, 512], replicated, may hold values from -6 to 6
- grad_edges: bfloat16 [65536, 512], P(('lat', 'blk')), may hold values from -6 to 6
Outputs:
- new_nodes: bfloat16 [10240, 512], P(('lat', 'blk'))
- new_coarse: bfloat16 [640, 512], replicated
- new_edges: bfloat16 [65536, 512], P(('lat', 'blk'))
- nodes_grad: bfloat16 [10240, 512], P(('lat', 'blk'))
- coarse_grad: bfloat16 [640, 512], replicated
- edges_grad: bfloat16 [65536, 512], P(('lat', 'blk'))
- edge_in_grad: bfloat16 [3, 512, 512], replicated
- edge_out_grad: bfloat16 [512, 512], replicated
- edge_gain_grad: float32 [512], replicated
- node_in_grad: bfloat16 [2, 512, 512], replicated
- node_out_grad: bfloat16 [512, 512], replicated
- node_gain_grad: float32 [512], replicated
The draws below stay inside these ranges and needn't reach their ends.
Inputs may be any that keep to these rules, and one draw needn't show every extreme that they name: `edge_tiles`: sender entries lie below 1024, receiver entries below 960. `send_lists`: numbers of nodes within the sending block. `tiles_live`: some block has all 16 tiles live.
All inputs are finite; a program needn't handle non-finite values.
Results may differ from the reference program's by a relative error of at most 0.0095.
Values may be sent and summed in bfloat16 or wider, within the bound.
A program may use at most 192 MiB of HBM per device.

```python
import jax
import jax.numpy as jnp
from jax import lax

D = 512
NODE_DEV = 320
TILE_DEV = 16
SLOTS = 8
NEIGH = 8
TILE = 128
COARSE = 640
BLOCKS = 32
NODES = 10240
TILES = 512
EDGES = 65536


def draw_edge_tiles(key, part):
    tile_shape = (TILES, TILE)
    subkeys = jax.random.split(jax.random.fold_in(key, 11), 7)
    sender_kind = jax.random.randint(subkeys[0], tile_shape, 0, 20)
    own_ids = jax.random.randint(subkeys[1], tile_shape, 0, NODE_DEV)
    halo_ids = NODE_DEV + jax.random.randint(subkeys[2], tile_shape, 0, NEIGH * SLOTS)
    coarse_ids = NODE_DEV + NEIGH * SLOTS + jax.random.randint(subkeys[3], tile_shape, 0, COARSE)
    senders = jnp.where(sender_kind < 10, own_ids, jnp.where(sender_kind < 17, halo_ids, coarse_ids))
    receiver_kind = jax.random.randint(subkeys[4], tile_shape, 0, 10)
    target_own = jax.random.randint(subkeys[5], tile_shape, 0, NODE_DEV)
    target_coarse = NODE_DEV + jax.random.randint(subkeys[6], tile_shape, 0, COARSE)
    receivers = jnp.where(receiver_kind < 9, target_own, target_coarse)
    return jnp.stack([senders, receivers], axis=1).astype(jnp.int32)


def draw_tiles_live(key, part):
    subkeys = jax.random.split(jax.random.fold_in(key, 23), 3)
    full_flag = jax.random.randint(subkeys[0], (BLOCKS,), 0, 8) == 0
    chosen = jax.random.randint(subkeys[1], (), 0, BLOCKS)
    partial_count = jax.random.randint(subkeys[2], (BLOCKS,), TILE_DEV // 2, TILE_DEV + 1)
    is_full = full_flag | (jnp.arange(BLOCKS) == chosen)
    return jnp.where(is_full, TILE_DEV, partial_count).astype(jnp.int32)


def plant(result, rng, smallest, largest):
    extent = result.shape
    spot = [jax.random.randint(jax.random.fold_in(rng, axis), (), 0, extent[axis]) for axis in range(len(extent))]
    result = result.at[tuple(spot)].set(smallest)
    longest = extent.index(max(extent))
    spot[longest] = (spot[longest] + 1) % extent[longest]
    return result.at[tuple(spot)].set(largest)


def shard_levels(key, extent, pieces, low, largest):
    def one(dim, parts):
        heights = jax.random.uniform(jax.random.fold_in(jax.random.fold_in(key, 6), dim), (parts,), jnp.float32, low / len(pieces), largest / len(pieces))
        return jnp.repeat(jnp.exp(heights), extent[dim] // parts).reshape((-1,) + (1,) * (len(extent) - dim - 1))

    loudness = one(*pieces[0])
    for cut in pieces[1:]:
        loudness = loudness * one(*cut)
    return loudness


def scatter_about(own_key, dims, deviation, reach, pieces=(), kind=jnp.bfloat16):
    loudness = shard_levels(own_key, dims, pieces, -0.22, 0.18) if pieces else 1.0
    result = jax.random.normal(own_key, dims, jnp.float32) * deviation * loudness
    return jnp.minimum(jnp.maximum(result, -reach), reach).astype(kind)


def setup_inputs(seed: int = 0) -> dict:
    seeds = jax.random.split(jax.random.key(seed), 16)
    return {
        "mesh_nodes": scatter_about(seeds[0], (NODES, D), 1.0, 6.0, ((0, 32),)),
        "coarse_nodes": scatter_about(seeds[1], (COARSE, D), 1.0, 6.0),
        "edge_latents": scatter_about(seeds[2], (EDGES, D), 1.0, 6.0, ((0, 32),)),
        "edge_tiles": draw_edge_tiles(jax.random.fold_in(seeds[15], 71), 0),
        "send_lists": plant(jax.random.randint(seeds[4], (BLOCKS, NEIGH, SLOTS), 0, NODE_DEV), jax.random.fold_in(seeds[4], 1), 0, NODE_DEV - 1).astype(jnp.int32),
        "tiles_live": draw_tiles_live(jax.random.fold_in(seeds[15], 71), 0),
        "edge_in": scatter_about(seeds[6], (3, D, D), (3 * D) ** -0.5, 0.15625),
        "edge_out": scatter_about(seeds[7], (D, D), D ** -0.5, 0.25),
        "edge_gain": jnp.clip(1.0 + 0.18 * jax.random.normal(seeds[8], (D,), jnp.float32), 0.1, 1.9),
        "node_in": scatter_about(seeds[9], (2, D, D), (2 * D) ** -0.5, 0.1875),
        "node_out": scatter_about(seeds[10], (D, D), D ** -0.5, 0.25),
        "node_gain": jnp.clip(1.0 + 0.18 * jax.random.normal(seeds[11], (D,), jnp.float32), 0.1, 1.9),
        "grad_nodes": scatter_about(seeds[12], (NODES, D), 1.0, 6.0, ((0, 32),)),
        "grad_coarse": scatter_about(seeds[13], (COARSE, D), 1.0, 6.0),
        "grad_edges": scatter_about(seeds[14], (EDGES, D), 1.0, 6.0, ((0, 32),)),
    }


EPS = 1e-05

def product(first_op, second_op):
    return jnp.dot(first_op, second_op, preferred_element_type=jnp.float32)

def inner_rows(first_op, second_op):
    return lax.dot_general(first_op, second_op, (((0,), (0,)), ((), ())), preferred_element_type=jnp.float32)

def outer_cols(first_op, second_op):
    return lax.dot_general(first_op, second_op, (((1,), (1,)), ((), ())), preferred_element_type=jnp.float32)

def exact_cols(first_op, second_op):
    return lax.dot_general(first_op, second_op, (((1,), (1,)), ((), ())), precision=lax.Precision.HIGHEST, preferred_element_type=jnp.float32)

def normalize(values):
    centered = values - lax.optimization_barrier(jnp.mean(values, axis=-1, keepdims=True))
    inverse = lax.rsqrt(lax.optimization_barrier(jnp.mean(centered * centered, axis=-1, keepdims=True)) + EPS)
    return (centered * inverse, inverse)

def normalize_back(upstream, normed, inverse):
    return inverse * (upstream - lax.optimization_barrier(jnp.mean(upstream, axis=-1, keepdims=True)) - normed * lax.optimization_barrier(jnp.mean(upstream * normed, axis=-1, keepdims=True)))

def swish_slope(values):
    sigmoid_v = jax.nn.sigmoid(values)
    return sigmoid_v * (1.0 + values * (1.0 - sigmoid_v))

def cycle_moves(neigh_count, block_count):
    near_count = neigh_count // 2 - 1
    near = [position - near_count for position in range(near_count)] + [position + 1 for position in range(near_count)]
    return near + [block_count // 4, block_count // 2]

def edge_forward(edge_rows, sender_part, receiver_part, alive_mask, edge_in, edge_out, edge_gain):
    preact = product(edge_rows, edge_in[0]) + sender_part + receiver_part
    hidden = jax.nn.silu(preact).astype(jnp.bfloat16)
    normed, inverse = normalize(product(hidden, edge_out))
    message = normed * edge_gain[None, :] * alive_mask[:, None]
    updated = (edge_rows.astype(jnp.float32) + message).astype(jnp.bfloat16)
    return (preact, hidden, normed, inverse, message, updated)

def edge_backward(edge_rows, preact, hidden, normed, inverse, alive_mask, message_grad, edge_in, edge_out, edge_gain):
    message_grad = message_grad * alive_mask[:, None]
    gain_grad = lax.optimization_barrier(jnp.sum(message_grad * normed, axis=0))
    out_slope = normalize_back(message_grad * edge_gain[None, :], normed, inverse).astype(jnp.bfloat16)
    out_grad = inner_rows(hidden, out_slope)
    pre_slope = (outer_cols(out_slope, edge_out) * swish_slope(preact)).astype(jnp.bfloat16)
    edge_grad = outer_cols(pre_slope, edge_in[0])
    first_grad = inner_rows(edge_rows, pre_slope)
    return (pre_slope, edge_grad, first_grad, out_grad, gain_grad)

def node_forward(node_rows, aggregate, node_in, node_out, node_gain):
    summed = aggregate.astype(jnp.bfloat16)
    preact = product(node_rows, node_in[0]) + product(summed, node_in[1])
    hidden = jax.nn.silu(preact).astype(jnp.bfloat16)
    normed, inverse = normalize(product(hidden, node_out))
    updated = (node_rows.astype(jnp.float32) + normed * node_gain[None, :]).astype(jnp.bfloat16)
    return (summed, preact, hidden, normed, inverse, updated)

def node_backward(node_rows, summed, preact, hidden, normed, inverse, node_slope, node_in, node_out, node_gain):
    gain_grad = lax.optimization_barrier(jnp.sum(node_slope * normed, axis=0))
    out_slope = normalize_back(node_slope * node_gain[None, :], normed, inverse).astype(jnp.bfloat16)
    out_grad = inner_rows(hidden, out_slope)
    pre_slope = (outer_cols(out_slope, node_out) * swish_slope(preact)).astype(jnp.bfloat16)
    direct = node_slope + outer_cols(pre_slope, node_in[0])
    aggregate_grad = outer_cols(pre_slope, node_in[1])
    in_grad = jnp.stack([inner_rows(node_rows, pre_slope), inner_rows(summed, pre_slope)])
    return (direct, aggregate_grad, in_grad, out_grad, gain_grad)

def reference(mesh_nodes, coarse_nodes, edge_latents, edge_tiles, send_lists, tiles_live, edge_in, edge_out, edge_gain, node_in, node_out, node_gain, grad_nodes, grad_coarse, grad_edges):
    block_count = tiles_live.shape[0]
    fine_count, features = mesh_nodes.shape
    node_dev = fine_count // block_count
    neigh_count = send_lists.shape[1]
    slot_count = send_lists.shape[2]
    halo_count = neigh_count * slot_count
    move_table = jnp.array(cycle_moves(neigh_count, block_count), dtype=jnp.int32)
    all_nodes = jnp.concatenate([mesh_nodes, coarse_nodes], axis=0)
    row_count = all_nodes.shape[0]
    sender_proj = product(all_nodes, edge_in[1])
    receiver_proj = product(all_nodes, edge_in[2])
    tile_dev = edge_tiles.shape[0] // block_count
    tile_width = edge_tiles.shape[2]
    edge_blocks = edge_latents.reshape(block_count, tile_dev * tile_width, features)
    tile_blocks = edge_tiles.reshape(block_count, tile_dev, 2, tile_width)
    slope_blocks = grad_edges.reshape(block_count, tile_dev * tile_width, features)
    block_ids = jnp.arange(block_count, dtype=jnp.int32)

    def endpoints(block, tiles):
        senders = tiles[:, 0, :].reshape(-1)
        receivers = tiles[:, 1, :].reshape(-1)
        offset = block * node_dev
        halo_pos = jnp.clip(senders - node_dev, 0, halo_count - 1).astype(jnp.int32)
        neighbour = (halo_pos // slot_count).astype(jnp.int32)
        moved_by = move_table[neighbour].astype(jnp.int32)
        source = ((block + moved_by) % block_count).astype(jnp.int32)
        listed = send_lists[source, neighbour, halo_pos % slot_count]
        sender_ids = jnp.where(senders < node_dev, offset + senders, jnp.where(senders < node_dev + halo_count, source * node_dev + listed, fine_count + senders - node_dev - halo_count))
        receiver_ids = jnp.where(receivers < node_dev, offset + receivers, fine_count + receivers - node_dev)
        alive_flag = jnp.arange(tile_dev, dtype=jnp.int32) < tiles_live[block]
        alive_mask = jnp.broadcast_to(alive_flag[:, None], (tile_dev, tile_width)).reshape(-1).astype(jnp.float32)
        return (sender_ids.astype(jnp.int32), receiver_ids.astype(jnp.int32), alive_mask)

    def forward_block(aggregate, block_data):
        block, edge_rows, tiles = block_data
        sender_ids, receiver_ids, alive_mask = endpoints(block, tiles)
        results = edge_forward(edge_rows, sender_proj[sender_ids], receiver_proj[receiver_ids], alive_mask, edge_in, edge_out, edge_gain)
        aggregate = aggregate + jax.ops.segment_sum(results[4], receiver_ids, num_segments=row_count)
        return (aggregate, results[5])
    zero_rows = jnp.zeros((row_count, features), jnp.float32)
    aggregate, new_edges = lax.scan(forward_block, zero_rows, (block_ids, edge_blocks, tile_blocks))
    summed, preact, hidden, normed, inverse, updated = node_forward(all_nodes, aggregate, node_in, node_out, node_gain)
    node_slope = jnp.concatenate([grad_nodes, grad_coarse], axis=0).astype(jnp.float32)
    direct, aggregate_grad, node_in_sum, node_out_sum, node_gain_sum = node_backward(all_nodes, summed, preact, hidden, normed, inverse, node_slope, node_in, node_out, node_gain)

    def backward_block(carry, block_data):
        sender_slope, receiver_slope, first_sum, sender_sum, receiver_sum, out_sum, gain_sum = carry
        block, edge_rows, tiles, edge_slope = block_data
        sender_ids, receiver_ids, alive_mask = endpoints(block, tiles)
        preact_e, hidden_e, normed_e, inverse_e, message, updated_e = edge_forward(edge_rows, sender_proj[sender_ids], receiver_proj[receiver_ids], alive_mask, edge_in, edge_out, edge_gain)
        message_grad = edge_slope.astype(jnp.float32) + aggregate_grad[receiver_ids]
        pre_slope, edge_grad, first_grad, out_grad, gain_grad = edge_backward(edge_rows, preact_e, hidden_e, normed_e, inverse_e, alive_mask, message_grad, edge_in, edge_out, edge_gain)
        sender_term = inner_rows(all_nodes[sender_ids], pre_slope)
        receiver_term = inner_rows(all_nodes[receiver_ids], pre_slope)
        wide_slope = lax.optimization_barrier(pre_slope).astype(jnp.float32)
        sender_slope = sender_slope + jax.ops.segment_sum(wide_slope, sender_ids, num_segments=row_count)
        receiver_slope = receiver_slope + jax.ops.segment_sum(wide_slope, receiver_ids, num_segments=row_count)
        carry = (sender_slope, receiver_slope, first_sum + first_grad, sender_sum + sender_term, receiver_sum + receiver_term, out_sum + out_grad, gain_sum + gain_grad)
        return (carry, (edge_slope.astype(jnp.float32) + edge_grad).astype(jnp.bfloat16))
    zero_square = jnp.zeros((features, features), jnp.float32)
    start_carry = (zero_rows, zero_rows, zero_square, zero_square, zero_square, zero_square, jnp.zeros((features,), jnp.float32))
    final_carry, edges_grad = lax.scan(backward_block, start_carry, (block_ids, edge_blocks, tile_blocks, slope_blocks))
    sender_slope, receiver_slope, first_sum, sender_sum, receiver_sum, out_sum, gain_sum = final_carry
    node_total = direct + exact_cols(sender_slope, edge_in[1].astype(jnp.float32)) + exact_cols(receiver_slope, edge_in[2].astype(jnp.float32))
    factor = float(edge_latents.shape[0]) ** (-0.5)
    edge_in_grad = (jnp.stack([first_sum, sender_sum, receiver_sum]) * factor).astype(jnp.bfloat16)
    return (updated[:fine_count], updated[fine_count:], new_edges.reshape(edge_latents.shape), node_total[:fine_count].astype(jnp.bfloat16), node_total[fine_count:].astype(jnp.bfloat16), edges_grad.reshape(edge_latents.shape), edge_in_grad, (out_sum * factor).astype(jnp.bfloat16), gain_sum * factor, (node_in_sum * factor).astype(jnp.bfloat16), (node_out_sum * factor).astype(jnp.bfloat16), node_gain_sum * factor)
```

```python
import functools

import jax
import jax.numpy as jnp
from jax import lax
from jax.experimental import pallas as pl
from jax.experimental.pallas import tpu as pltpu
from jax.sharding import PartitionSpec as P

EPS = 1e-05
BF = jnp.bfloat16
F32 = jnp.float32
AXES = ("lat", "blk")


def dims(a, b, ca, cb):
    return lax.dot_general(a, b, (((ca,), (cb,)), ((), ())), preferred_element_type=F32)


def product(a, b):
    return dims(a, b, 1, 0)


def inner_rows(a, b):
    return dims(a, b, 0, 0)


def outer_cols(a, b):
    return dims(a, b, 1, 1)


def normalize(values):
    centered = values - jnp.mean(values, axis=-1, keepdims=True)
    inverse = lax.rsqrt(jnp.mean(centered * centered, axis=-1, keepdims=True) + EPS)
    return (centered * inverse, inverse)


def normalize_back(upstream, normed, inverse):
    return inverse * (
        upstream
        - jnp.mean(upstream, axis=-1, keepdims=True)
        - normed * jnp.mean(upstream * normed, axis=-1, keepdims=True)
    )


def one_hot(index, shape, axis):
    return jnp.where(lax.broadcasted_iota(jnp.int32, shape, axis) == index, 1.0, 0.0).astype(BF)


def cycle_moves(neigh_count, block_count):
    near_count = neigh_count // 2 - 1
    near = [position - near_count for position in range(near_count)] + [
        position + 1 for position in range(near_count)
    ]
    return near + [block_count // 4, block_count // 2]


def edge_forward(
    tile_width,
    live_ref,
    lat_ref,
    send_col,
    recv_col,
    recv_row,
    mesh_ref,
    halo_ref,
    coarse_ref,
    win_ref,
    wout_ref,
    gain_ref,
    new_ref,
    hid_ref,
    slope_ref,
    norm_ref,
    inv_ref,
    agg_own,
    agg_coarse,
    proj_s,
    proj_r,
    agg,
):
    step = pl.program_id(0)
    own, halo = mesh_ref.shape[0], halo_ref.shape[0]
    rows = agg.shape[0]
    block = lat_ref.shape[0]

    @pl.when(step == 0)
    def _():
        agg[...] = jnp.zeros_like(agg)
        for part, lo in ((mesh_ref, 0), (halo_ref, own), (coarse_ref, own + halo)):
            span = pl.ds(lo, part.shape[0])
            proj_s[span, :] = product(part[...], win_ref[1]).astype(BF)
            proj_r[span, :] = product(part[...], win_ref[2]).astype(BF)

    rows_in = lat_ref[...]
    pre = (
        product(rows_in, win_ref[0])
        + product(one_hot(send_col[...], (block, rows), 1), proj_s[...])
        + product(one_hot(recv_col[...], (block, rows), 1), proj_r[...])
    )
    sig = 1.0 / (1.0 + jnp.exp(-pre))
    hidden = (pre * sig).astype(BF)
    slope_ref[...] = (sig * (1.0 + pre * (1.0 - sig))).astype(BF)
    hid_ref[...] = hidden
    normed, inverse = normalize(product(hidden, wout_ref[...]))
    norm_ref[...] = normed.astype(BF)
    inv_ref[...] = inverse
    place = step * block + lax.broadcasted_iota(jnp.int32, (block, 1), 0)
    alive = jnp.where(place < live_ref[0] * tile_width, 1.0, 0.0)
    message = normed * gain_ref[...] * alive
    new_ref[...] = (rows_in.astype(F32) + message).astype(BF)
    agg[...] += product(one_hot(recv_row[...], (rows, block), 0), message.astype(BF))

    @pl.when(step == pl.num_programs(0) - 1)
    def _():
        agg_own[...] = agg[pl.ds(0, own), :].astype(BF)
        agg_coarse[...] = agg[pl.ds(own + halo, rows - own - halo), :].astype(BF)


def edge_backward(
    tile_width,
    live_ref,
    lat_ref,
    grad_ref,
    hid_ref,
    slope_ref,
    norm_ref,
    inv_ref,
    recv_col,
    recv_row,
    send_row,
    mesh_ref,
    halo_ref,
    coarse_ref,
    own_slope,
    coarse_slope,
    win_ref,
    wout_ref,
    gain_ref,
    edges_grad,
    in_grad,
    out_grad,
    gain_grad,
    own_term,
    halo_term,
    coarse_term,
    table,
    sent,
    received,
    first_acc,
    out_acc,
):
    step = pl.program_id(0)
    own, halo = mesh_ref.shape[0], halo_ref.shape[0]
    rows = table.shape[0]
    block = lat_ref.shape[0]

    @pl.when(step == 0)
    def _():
        for acc in (sent, received, first_acc, out_acc, gain_grad):
            acc[...] = jnp.zeros_like(acc)
        table[pl.ds(0, own), :] = own_slope[...]
        table[pl.ds(own, halo), :] = jnp.zeros((halo, table.shape[1]), BF)
        table[pl.ds(own + halo, rows - own - halo), :] = coarse_slope[...]

    place = step * block + lax.broadcasted_iota(jnp.int32, (block, 1), 0)
    alive = jnp.where(place < live_ref[0] * tile_width, 1.0, 0.0)
    edge_slope = grad_ref[...].astype(F32)
    message_slope = (
        edge_slope + product(one_hot(recv_col[...], (block, rows), 1), table[...])
    ) * alive
    normed = norm_ref[...].astype(F32)
    gain_grad[...] += jnp.sum(message_slope * normed, axis=0, keepdims=True)
    out_slope = normalize_back(message_slope * gain_ref[...], normed, inv_ref[...]).astype(BF)
    out_acc[...] += inner_rows(hid_ref[...], out_slope)
    pre_slope = (outer_cols(out_slope, wout_ref[...]) * slope_ref[...].astype(F32)).astype(BF)
    edges_grad[...] = (edge_slope + outer_cols(pre_slope, win_ref[0])).astype(BF)
    first_acc[...] += inner_rows(lat_ref[...], pre_slope)
    sent[...] += product(one_hot(send_row[...], (rows, block), 0), pre_slope)
    received[...] += product(one_hot(recv_row[...], (rows, block), 0), pre_slope)

    @pl.when(step == pl.num_programs(0) - 1)
    def _():
        in_grad[0] = first_acc[...].astype(BF)
        out_grad[...] = out_acc[...].astype(BF)
        sums = [None, None]
        for part, lo, term in (
            (mesh_ref, 0, own_term),
            (halo_ref, own, halo_term),
            (coarse_ref, own + halo, coarse_term),
        ):
            span = pl.ds(lo, part.shape[0])
            total = None
            for which, source in enumerate((sent, received)):
                piece = source[span, :].astype(BF)
                weight = inner_rows(part[...], piece)
                sums[which] = weight if sums[which] is None else sums[which] + weight
                back = outer_cols(piece, win_ref[1 + which])
                total = back if total is None else total + back
            term[...] = total.astype(term.dtype)
        in_grad[1] = sums[0].astype(BF)
        in_grad[2] = sums[1].astype(BF)


def node_step(
    rows_ref,
    sum_ref,
    grad_ref,
    win_ref,
    wout_ref,
    gain_ref,
    new_ref,
    direct_ref,
    agg_grad,
    in_grad,
    out_grad,
    gain_grad,
):
    @pl.when(pl.program_id(0) == 0)
    def _():
        for acc in (in_grad, out_grad, gain_grad):
            acc[...] = jnp.zeros_like(acc)

    rows = rows_ref[...]
    summed = sum_ref[...]
    pre = product(rows, win_ref[0]) + product(summed, win_ref[1])
    sig = 1.0 / (1.0 + jnp.exp(-pre))
    hidden = (pre * sig).astype(BF)
    normed, inverse = normalize(product(hidden, wout_ref[...]))
    new_ref[...] = (rows.astype(F32) + normed * gain_ref[...]).astype(BF)
    node_slope = grad_ref[...].astype(F32)
    gain_grad[...] += jnp.sum(node_slope * normed, axis=0, keepdims=True)
    out_slope = normalize_back(node_slope * gain_ref[...], normed, inverse).astype(BF)
    out_grad[...] += inner_rows(hidden, out_slope)
    swish = sig * (1.0 + pre * (1.0 - sig))
    pre_slope = (outer_cols(out_slope, wout_ref[...]) * swish).astype(BF)
    direct_ref[...] = node_slope + outer_cols(pre_slope, win_ref[0])
    agg_grad[...] = outer_cols(pre_slope, win_ref[1]).astype(BF)
    in_grad[0] += inner_rows(rows, pre_slope)
    in_grad[1] += inner_rows(summed, pre_slope)


def whole(shape):
    zero = (0,) * len(shape)
    return pl.BlockSpec(shape, lambda i: zero)


def by_rows(block, width):
    return pl.BlockSpec((block, width), lambda i: (i, 0))


def by_cols(block):
    return pl.BlockSpec((1, block), lambda i: (0, i))


def shape_of(shape, dtype):
    return jax.ShapeDtypeStruct(shape, dtype)


def cost(flops, moved):
    return pl.CostEstimate(flops=int(flops), bytes_accessed=int(moved), transcendentals=0)


PARAMS = dict(
    compiler_params=pltpu.CompilerParams(
        dimension_semantics=("arbitrary",), vmem_limit_bytes=60 * 1024 * 1024
    )
)


def node_call(rows, summed, grad, node_in, node_out, gain, block):
    count, d = rows.shape
    row = by_rows(block, d)
    return pl.pallas_call(
        node_step,
        grid=(count // block,),
        in_specs=[row, row, row, whole((2, d, d)), whole((d, d)), whole((1, d))],
        out_specs=[row, row, row, whole((2, d, d)), whole((d, d)), whole((1, d))],
        out_shape=[
            shape_of((count, d), BF),
            shape_of((count, d), F32),
            shape_of((count, d), BF),
            shape_of((2, d, d), F32),
            shape_of((d, d), F32),
            shape_of((1, d), F32),
        ],
        cost_estimate=cost(18 * count * d * d, 12 * count * d),
        **PARAMS,
    )(rows, summed, grad, node_in, node_out, gain)


def on_device(
    mesh_nodes,
    coarse_nodes,
    edge_latents,
    edge_tiles,
    send_lists,
    tiles_live,
    edge_in,
    edge_out,
    edge_gain,
    node_in,
    node_out,
    node_gain,
    grad_nodes,
    grad_coarse,
    grad_edges,
):
    block_count = lax.axis_size("lat") * lax.axis_size("blk")
    own, d = mesh_nodes.shape
    neigh, slots = send_lists.shape[1:]
    coarse = coarse_nodes.shape[0]
    halo = neigh * slots
    rows = own + halo + coarse
    tile_dev, _, tile_width = edge_tiles.shape
    edges = tile_dev * tile_width
    block = 4 * tile_width if tile_dev % 4 == 0 else tile_width
    moves = cycle_moves(neigh, block_count)
    listed = send_lists[0].reshape(-1)
    pick = (listed[:, None] == jnp.arange(own, dtype=jnp.int32)[None, :]).astype(BF)
    outgoing = product(pick, mesh_nodes).astype(BF).reshape(neigh, slots, d)

    def exchange(pieces, sign):
        got = []
        for k, move in enumerate(moves):
            pairs = [(b, (b + sign * move) % block_count) for b in range(block_count)]
            got.append(lax.ppermute(pieces[k], AXES, pairs))
        return jnp.concatenate(got, axis=0)

    incoming = exchange(outgoing, -1)
    senders = edge_tiles[:, 0, :].reshape(-1)
    receivers = edge_tiles[:, 1, :].reshape(-1)
    receivers = jnp.where(receivers < own, receivers, receivers + halo)
    send_row, recv_row = senders.reshape(1, edges), receivers.reshape(1, edges)
    send_col, recv_col = senders.reshape(edges, 1), receivers.reshape(edges, 1)
    e_gain, n_gain = edge_gain.reshape(1, d), node_gain.reshape(1, d)

    smem = pl.BlockSpec(memory_space=pltpu.SMEM)
    wide, col, row = by_rows(block, d), by_rows(block, 1), by_cols(block)
    tables = [whole((own, d)), whole((halo, d)), whole((coarse, d))]
    weights = [whole((3, d, d)), whole((d, d)), whole((1, d))]
    new_edges, hidden, slope, normed, inverse, agg_own, agg_coarse = pl.pallas_call(
        functools.partial(edge_forward, tile_width),
        grid=(edges // block,),
        in_specs=[smem, wide, col, col, row] + tables + weights,
        out_specs=[wide] * 4 + [col, whole((own, d)), whole((coarse, d))],
        out_shape=[shape_of((edges, d), BF)] * 4
        + [shape_of((edges, 1), F32), shape_of((own, d), BF), shape_of((coarse, d), BF)],
        scratch_shapes=[
            pltpu.VMEM((rows, d), BF),
            pltpu.VMEM((rows, d), BF),
            pltpu.VMEM((rows, d), F32),
        ],
        cost_estimate=cost(2 * edges * d * (3 * rows + 2 * d), 12 * edges * d),
        **PARAMS,
    )(
        tiles_live,
        edge_latents,
        send_col,
        recv_col,
        recv_row,
        mesh_nodes,
        incoming,
        coarse_nodes,
        edge_in,
        edge_out,
        e_gain,
    )
    coarse_total = lax.psum(agg_coarse, AXES)
    new_nodes, own_direct, own_slope, own_in, own_out, own_ngain = node_call(
        mesh_nodes, agg_own, grad_nodes, node_in, node_out, n_gain, own
    )
    c_block = own if coarse % own == 0 else coarse
    new_coarse, c_direct, c_slope, c_in, c_out, c_ngain = node_call(
        coarse_nodes, coarse_total, grad_coarse, node_in, node_out, n_gain, c_block
    )
    node_sums = lax.psum((own_in.astype(BF), own_out.astype(BF)), AXES)
    edges_grad, in_grad, out_grad, gain_grad, own_term, halo_term, coarse_term = pl.pallas_call(
        functools.partial(edge_backward, tile_width),
        grid=(edges // block,),
        in_specs=[smem] + [wide] * 5 + [col, col, row, row] + tables
        + [whole((own, d)), whole((coarse, d))] + weights,
        out_specs=[wide, whole((3, d, d)), whole((d, d)), whole((1, d))] + tables,
        out_shape=[
            shape_of((edges, d), BF),
            shape_of((3, d, d), BF),
            shape_of((d, d), BF),
            shape_of((1, d), F32),
            shape_of((own, d), F32),
            shape_of((halo, d), BF),
            shape_of((coarse, d), BF),
        ],
        scratch_shapes=[
            pltpu.VMEM((rows, d), BF),
            pltpu.VMEM((rows, d), F32),
            pltpu.VMEM((rows, d), F32),
            pltpu.VMEM((d, d), F32),
            pltpu.VMEM((d, d), F32),
        ],
        cost_estimate=cost(2 * edges * d * (3 * rows + 4 * d), 14 * edges * d),
        **PARAMS,
    )(
        tiles_live,
        edge_latents,
        grad_edges,
        hidden,
        slope,
        normed,
        inverse,
        recv_col,
        recv_row,
        send_row,
        mesh_nodes,
        incoming,
        coarse_nodes,
        own_slope,
        c_slope,
        edge_in,
        edge_out,
        e_gain,
    )
    gains = jnp.concatenate([gain_grad, own_ngain], axis=0).astype(BF)
    sums_in, sums_out, coarse_back, gain_sums = lax.psum(
        (in_grad, out_grad, coarse_term, gains), AXES
    )
    returned = exchange(halo_term.reshape(neigh, slots, d), 1)
    own_total = own_direct + own_term + inner_rows(pick, returned)
    factor = float(edges * block_count) ** (-0.5)
    return (
        new_nodes,
        new_coarse,
        new_edges,
        own_total.astype(BF),
        (c_direct + coarse_back.astype(F32)).astype(BF),
        edges_grad,
        (sums_in.astype(F32) * factor).astype(BF),
        (sums_out.astype(F32) * factor).astype(BF),
        gain_sums[0].astype(F32) * factor,
        ((node_sums[0].astype(F32) + c_in) * factor).astype(BF),
        ((node_sums[1].astype(F32) + c_out) * factor).astype(BF),
        (gain_sums[1].astype(F32) + c_ngain[0]) * factor,
    )


def solution(mesh):
    rows2 = P(AXES, None)
    rows3 = P(AXES, None, None)
    in_specs = (
        rows2, P(), rows2, rows3, rows3, P(AXES), P(), P(), P(), P(), P(), P(), rows2, P(), rows2,
    )
    out_specs = (rows2, P(), rows2, rows2, P(), rows2, P(), P(), P(), P(), P(), P())
    return jax.shard_map(
        on_device, mesh=mesh, in_specs=in_specs, out_specs=out_specs, check_vma=False
    )
```
